32 devices in a mesh: section: 2 (over x), tensor: 4 (over z), dp: 4 (over y, core).
Axes of the slice: x: 2, y: 2, z: 4, core: 2. Of those that a mesh axis runs over, the one named last changes fastest.
Arguments:
- tokens: bfloat16 [16, 4096], P(None, ('section', 'dp')), may hold values from -100 to 100
- attn_gain: float32 [4096], P(('section', 'dp')), may hold values from 0.1 to 1.9
- qkv_weight: bfloat16 [4096, 10240], P(('section', 'dp'), 'tensor'), may hold values from -0.09375 to 0.09375
- qkv_order: int32 [10], replicated, may hold values from 0 to 9, each once
- cache_keys: bfloat16 [16, 8, 4096, 128], P(('section', 'dp'), 'tensor'), may hold values from -1300 to 1300
- cache_values: bfloat16 [16, 8, 4096, 128], P(('section', 'dp'), 'tensor'), may hold values from -6 to 6
- cache_len: int32 [16], P(('section', 'dp')), may hold values from 2 to 4096, as said below
- out_weight: bfloat16 [8192, 4096], P('tensor', ('section', 'dp')), may hold values from -0.0625 to 0.0625
- ffn_gain: float32 [4096], P(('section', 'dp')), may hold values from 0.1 to 1.9
- gate_up: bfloat16 [2, 4096, 28672], P(None, ('section', 'dp'), 'tensor'), may hold values from -0.09375 to 0.09375
- down_weight: bfloat16 [28672, 4096], P('tensor', ('section', 'dp')), may hold values from -0.03125 to 0.03125
Outputs:
- layer_out: bfloat16 [16, 4096], P(None, ('section', 'dp'))
The draws below stay inside these ranges and needn't reach their ends.
Inputs may be any that keep to these rules, and one draw needn't show every extreme that they name: qkv_order is a permutation of 0 to 9, the same for every key-value group. `cache_len`: at least one sequence has all 4096 positions valid.
All inputs are finite; a program needn't handle non-finite values.
Results may differ from the reference program's by a relative error of at most 0.0065.
Values may be sent and summed in bfloat16 or wider, within the bound.
A program may use at most 64 MiB of HBM per device.

```python
import math
import jax
import jax.numpy as jnp
from jax import lax

D = 4096
HEADS = 64
KV_HEADS = 8
HD = 128
FF = 28672
LEN = 4096
GROUP = 10
B = 16


def draw_tokens(key, part):
    key_base, key_rows, key_cols = jax.random.split(key, 3)
    normal_part = jnp.clip(jax.random.normal(key_base, (B, D), jnp.float32), -4.0, 4.0)
    column_scale = 3.0 ** (jnp.arange(D, dtype=jnp.float32) / (D - 1))
    column_scale = column_scale * jnp.exp(jax.random.uniform(key_cols, (1, D), jnp.float32, -0.35, 0.35))
    row_scale = jnp.exp(jax.random.uniform(key_rows, (B, 1), jnp.float32, math.log(0.3), math.log(3.0)))
    return (normal_part * row_scale * column_scale).astype(jnp.bfloat16)


def draw_cache_keys(key, part):
    key_base = jax.random.fold_in(key, 0)
    base_keys = 2.5 * jnp.clip(jax.random.normal(key_base, (B, KV_HEADS, LEN, HD), jnp.float32), -6.0, 6.0)
    return base_keys.astype(jnp.bfloat16)


def draw_cache_len(key, part):
    lengths = jax.random.randint(key, (B,), 2, LEN + 1, dtype=jnp.int32)
    return lengths.at[0].set(LEN)


def shard_levels(own_key, extent, cuts, low, top_value):
    factor_of = 1.0
    for axis_at, parts in cuts:
        draws = jax.random.uniform(jax.random.fold_in(jax.random.fold_in(own_key, 6), axis_at), (parts,), jnp.float32, low / len(cuts), top_value / len(cuts))
        factor_of = factor_of * jnp.repeat(jnp.exp(draws), extent[axis_at] // parts).reshape((-1,) + (1,) * (len(extent) - 1 - axis_at))
    return factor_of


def gaussian(key, dims, scale, reach, shards=(), held_as=jnp.bfloat16):
    drawn = jax.random.normal(key, dims, jnp.float32) * scale
    if len(shards) > 0:
        drawn = shard_levels(key, dims, shards, -0.22, 0.18) * drawn
    return jnp.clip(drawn, min=-reach, max=reach).astype(held_as)


def setup_inputs(seed: int = 0) -> dict:
    seeds = jax.random.split(jax.random.key(seed), 12)
    tokens = draw_tokens(jax.random.fold_in(seeds[11], 71), 0)
    attn_gain = jnp.clip(1.0 + 0.18 * jax.random.normal(seeds[1], (D,), jnp.float32), 0.1, 1.9)
    qkv_weight = gaussian(seeds[2], (D, KV_HEADS * GROUP * HD), D ** -0.5, 0.09375, ((0, 8), (1, 4)))
    qkv_order = jax.random.permutation(seeds[3], GROUP).astype(jnp.int32)
    cache_keys = draw_cache_keys(jax.random.fold_in(seeds[11], 71), 0)
    cache_values = gaussian(seeds[5], (B, KV_HEADS, LEN, HD), 1.0, 6.0, ((0, 8), (1, 4)))
    cache_len = draw_cache_len(jax.random.fold_in(seeds[11], 71), 0)
    out_weight = gaussian(seeds[7], (HEADS * HD, D), (HEADS * HD) ** -0.5, 0.0625, ((0, 4), (1, 8)))
    ffn_gain = jnp.clip(1.0 + 0.18 * jax.random.normal(seeds[8], (D,), jnp.float32), 0.1, 1.9)
    gate_up = gaussian(seeds[9], (2, D, FF), D ** -0.5, 0.09375, ((1, 8), (2, 4)))
    down_weight = gaussian(seeds[10], (FF, D), FF ** -0.5, 0.03125, ((0, 4), (1, 8)))
    return dict(tokens=tokens, attn_gain=attn_gain, qkv_weight=qkv_weight, qkv_order=qkv_order, cache_keys=cache_keys, cache_values=cache_values, cache_len=cache_len, out_weight=out_weight, ffn_gain=ffn_gain, gate_up=gate_up, down_weight=down_weight)


def normalize(stream, gain_vec):
    wide = stream.astype(jnp.float32)
    meansq = lax.optimization_barrier(jnp.mean(wide * wide, axis=-1, keepdims=True))
    return (wide * lax.rsqrt(meansq + 1e-05) * gain_vec.astype(jnp.float32)).astype(jnp.bfloat16)

def rotate(vector, cosine, sine_part):
    half_dim = vector.shape[-1] // 2
    first_half = vector[..., :half_dim]
    second = vector[..., half_dim:]
    return jnp.concatenate([first_half * cosine - second * sine_part, second * cosine + first_half * sine_part], axis=-1)

def attend_one(packed):
    queries, new_key, new_value, key_cache, value_cache, length = packed
    inv_scale = 1.0 / jnp.sqrt(jnp.float32(HD))
    scores = jnp.einsum('gpd,gld->gpl', queries.astype(jnp.float32), key_cache.astype(jnp.float32)) * inv_scale
    own_score = jnp.einsum('gpd,gd->gp', queries.astype(jnp.float32), new_key.astype(jnp.float32)) * inv_scale
    valid_mask = jnp.arange(LEN, dtype=jnp.int32) < length
    masked = jnp.where(valid_mask[None, None, :], scores, -jnp.inf)
    peak = jnp.maximum(lax.optimization_barrier(jnp.max(masked, axis=-1)), own_score)
    weights = jnp.exp(masked - peak[..., None])
    own_weight = jnp.exp(own_score - peak)
    denom_sum = lax.optimization_barrier(jnp.sum(weights, axis=-1)) + own_weight
    probabilities = (weights / denom_sum[..., None]).astype(jnp.bfloat16)
    own_prob = (own_weight / denom_sum).astype(jnp.bfloat16)
    mixed_heads = jnp.einsum('gpl,gld->gpd', probabilities.astype(jnp.float32), value_cache.astype(jnp.float32))
    mixed_heads = mixed_heads + own_prob.astype(jnp.float32)[..., None] * new_value.astype(jnp.float32)[:, None, :]
    return mixed_heads.astype(jnp.bfloat16).reshape(-1)

def reference(tokens, attn_gain, qkv_weight, qkv_order, cache_keys, cache_values, cache_len, out_weight, ffn_gain, gate_up, down_weight):
    per_group = HEADS // KV_HEADS
    normed = normalize(tokens, attn_gain)
    joined_cols = jnp.dot(normed, qkv_weight, preferred_element_type=jnp.float32)
    blocks = joined_cols.reshape(B, KV_HEADS, GROUP, HD)
    onehot = (qkv_order[:, None] == jnp.arange(GROUP, dtype=jnp.int32)[None, :]).astype(jnp.float32)
    logical = jnp.einsum('bgjd,ji->bgid', blocks, onehot, precision=lax.Precision.HIGHEST)
    half_dim = HD // 2
    inv_freq = 500000.0 ** (-(2.0 * jnp.arange(half_dim, dtype=jnp.float32)) / HD)
    angles = cache_len.astype(jnp.float32)[:, None] * inv_freq[None, :]
    cosine = jnp.cos(angles)
    sine_part = jnp.sin(angles)
    queries = rotate(logical[:, :, :per_group], cosine[:, None, None, :], sine_part[:, None, None, :]).astype(jnp.bfloat16)
    new_key = rotate(logical[:, :, per_group], cosine[:, None, :], sine_part[:, None, :]).astype(jnp.bfloat16)
    new_value = logical[:, :, per_group + 1].astype(jnp.bfloat16)
    attended = lax.map(attend_one, (queries, new_key, new_value, cache_keys, cache_values, cache_len))
    projected = jnp.dot(attended, out_weight, preferred_element_type=jnp.float32)
    hidden_state = (tokens.astype(jnp.float32) + projected).astype(jnp.bfloat16)
    ffn_normed = normalize(hidden_state, ffn_gain)
    gate = jnp.dot(ffn_normed, gate_up[0], preferred_element_type=jnp.float32)
    upward = jnp.dot(ffn_normed, gate_up[1], preferred_element_type=jnp.float32)
    activated = (jax.nn.silu(gate) * upward).astype(jnp.bfloat16)
    lowered = jnp.dot(activated, down_weight, preferred_element_type=jnp.float32)
    return (hidden_state.astype(jnp.float32) + lowered).astype(jnp.bfloat16)
```

```python
import functools
import math

import jax
import jax.numpy as jnp
from jax import lax
from jax.experimental import pallas as pl
from jax.experimental.pallas import tpu as pltpu
from jax.sharding import PartitionSpec as P

MESH = pl.DeviceIdType.MESH
F32 = jnp.float32
BF16 = jnp.bfloat16
NT = (((1,), (1,)), ((), ()))


def layer_kernel(
    dims,
    order,
    lens,
    tokens,
    gain1,
    gain2,
    cos_full,
    sin_full,
    wq_hbm,
    ck_hbm,
    cv_hbm,
    wo_hbm,
    wgu_hbm,
    wd_hbm,
    out,
    wq,
    ck,
    cv,
    wo,
    wgu,
    wd,
    load_sem,
    qsend,
    qrecv,
    lbuf,
    att,
    heads_all,
    heads_full,
    zsend,
    zrecv,
    hidden,
    scaled,
    ssend,
    srecv,
    gsend,
    grecv,
    asend,
    act_all,
    down_acc,
    q_ss,
    q_rs,
    h_ss,
    h_rs,
    z_ss,
    z_rs,
    s_ss,
    s_rs,
    g_ss,
    g_rs,
    a_ss,
    a_rs,
):
    n_section, n_dp, n_tensor = dims
    group = n_section * n_dp
    me = lax.axis_index("section") * n_dp + lax.axis_index("dp")
    t_me = lax.axis_index("tensor")
    rows, width = tokens.shape
    full_width = width * group
    seqs, groups, length, hd = ck.shape
    qcols = wq.shape[1]
    blocks = qcols // (groups * hd)
    per_group = blocks - 2
    n_row, row_part = scaled.shape[0], scaled.shape[1]
    n_col = group // n_row
    piece = asend.shape[1]

    def plane(index):
        return {"section": index // n_dp, "dp": index % n_dp}

    loads = [
        pltpu.make_async_copy(src, dst, load_sem.at[i])
        for i, (src, dst) in enumerate(
            (
                (wq_hbm, wq),
                (ck_hbm, ck),
                (cv_hbm, cv),
                (wo_hbm, wo),
                (wgu_hbm, wgu),
                (wd_hbm, wd),
            )
        )
    ]
    loads[0].start()
    loads[1].start()

    barrier = pltpu.get_barrier_semaphore()
    for k in range(1, group):
        pl.semaphore_signal(
            barrier, inc=1, device_id=plane(lax.rem(me + k, group)), device_id_type=MESH
        )
    for k in range(1, n_tensor):
        pl.semaphore_signal(
            barrier, inc=1, device_id={"tensor": lax.rem(t_me + k, n_tensor)}, device_id_type=MESH
        )

    x = tokens[...].astype(F32)
    squares = jnp.sum(x * x, axis=1, keepdims=True)
    xg = (x * gain1[...]).astype(BF16)
    loads[0].wait()
    for load in loads[2:]:
        load.start()
    part = jnp.dot(xg, wq[...], preferred_element_type=F32)
    sq_lanes = jnp.broadcast_to(squares, (rows, hd))
    for p in range(group):
        qsend[p, :, :qcols] = part[p * seqs : (p + 1) * seqs]
        qsend[p, :, qcols:] = sq_lanes[p * seqs : (p + 1) * seqs]
    pl.semaphore_wait(barrier, group - 1 + n_tensor - 1)

    def q_copy(k):
        to = lax.rem(me + k, group)
        return pltpu.make_async_remote_copy(
            src_ref=qsend.at[to],
            dst_ref=qrecv.at[k - 1],
            send_sem=q_ss.at[k - 1],
            recv_sem=q_rs.at[k - 1],
            device_id=plane(to),
            device_id_type=MESH,
        )

    for k in range(1, group):
        q_copy(k).start()
    total = qsend[me]
    for k in range(1, group):
        q_copy(k).wait_recv()
        total = total + qrecv[k - 1]
    factor = lax.rsqrt(total[:, qcols:] / full_width + 1e-05)
    for g in range(groups):
        stored = [
            total[:, (g * blocks + j) * hd : (g * blocks + j + 1) * hd] * factor
            for j in range(blocks)
        ]
        for i in range(blocks):
            logical = jnp.zeros((seqs, hd), F32)
            for j in range(blocks):
                logical = logical + jnp.where(order[j] == i, 1.0, 0.0).astype(F32) * stored[j]
            for b in range(seqs):
                lbuf[b, g, i : i + 1, :] = logical[b : b + 1]

    loads[1].wait()
    loads[2].wait()
    inv_scale = 1.0 / math.sqrt(hd)
    column = lax.broadcasted_iota(jnp.int32, (per_group, length), 1)

    def turn(vec, b):
        return vec * cos_full[b : b + 1, :] + pltpu.roll(vec, hd // 2, 1) * sin_full[b : b + 1, :]

    for b in range(seqs):
        for g in range(groups):
            q = turn(lbuf[b, g, :per_group, :], b).astype(BF16)
            both = lbuf[b, g, per_group : per_group + 8, :]
            nk = turn(both, b).astype(BF16).astype(F32)[0:1]
            nv = both.astype(BF16).astype(F32)[1:2]
            scores = lax.dot_general(q, ck[b, g], NT, preferred_element_type=F32) * inv_scale
            own = jnp.sum(q.astype(F32) * nk, axis=1, keepdims=True) * inv_scale
            scores = jnp.where(column < lens[b], scores, -jnp.inf)
            peak = jnp.maximum(jnp.max(scores, axis=1, keepdims=True), own)
            weights = jnp.exp(scores - peak)
            own_w = jnp.exp(own - peak)
            denom = jnp.sum(weights, axis=1, keepdims=True) + own_w
            mixed = jnp.dot(weights.astype(BF16), cv[b, g], preferred_element_type=F32)
            mixed = (mixed + own_w * nv) / denom
            for i in range(per_group):
                at = (g * per_group + i) * hd
                att[b : b + 1, at : at + hd] = mixed[i : i + 1]

    def h_copy(k):
        return pltpu.make_async_remote_copy(
            src_ref=att,
            dst_ref=heads_all.at[me],
            send_sem=h_ss.at[k - 1],
            recv_sem=h_rs.at[k - 1],
            device_id=plane(lax.rem(me + k, group)),
            device_id_type=MESH,
        )

    for k in range(1, group):
        h_copy(k).start()
    heads_all[me] = att[...]
    loads[3].wait()
    for k in range(1, group):
        h_copy(k).wait_recv()
    for p in range(group):
        heads_full[p * seqs : (p + 1) * seqs, :] = heads_all[p]

    def z_copy(stage, k):
        return pltpu.make_async_remote_copy(
            src_ref=zsend.at[stage],
            dst_ref=zrecv.at[stage, t_me],
            send_sem=z_ss.at[stage, k - 1],
            recv_sem=z_rs.at[stage, k - 1],
            device_id={"tensor": lax.rem(t_me + k, n_tensor)},
            device_id_type=MESH,
        )

    def tensor_sum(stage, partial):
        rounded = partial.astype(BF16)
        zsend[stage] = rounded
        for k in range(1, n_tensor):
            z_copy(stage, k).start()
        zrecv[stage, t_me] = rounded
        for k in range(1, n_tensor):
            z_copy(stage, k).wait_recv()
        summed = zrecv[stage, 0].astype(F32)
        for t in range(1, n_tensor):
            summed = summed + zrecv[stage, t].astype(F32)
        return summed

    partial = jnp.dot(heads_full[...].astype(BF16), wo[...], preferred_element_type=F32)
    state = (tokens[...].astype(F32) + tensor_sum(0, partial)).astype(BF16)
    hidden[...] = state
    h32 = state.astype(F32)
    hsq = jnp.broadcast_to(jnp.sum(h32 * h32, axis=1, keepdims=True), (rows, hd))
    hgain = (h32 * gain2[...]).astype(BF16)
    for r in range(n_row):
        ssend[r] = hsq[r * row_part : (r + 1) * row_part]
        scaled[r] = hgain[r * row_part : (r + 1) * row_part]

    def s_copy(k):
        return pltpu.make_async_remote_copy(
            src_ref=ssend,
            dst_ref=srecv.at[k - 1],
            send_sem=s_ss.at[k - 1],
            recv_sem=s_rs.at[k - 1],
            device_id=plane(lax.rem(me + k, group)),
            device_id_type=MESH,
        )

    for k in range(1, group):
        s_copy(k).start()

    loads[4].wait()

    def g_copy(k):
        return pltpu.make_async_remote_copy(
            src_ref=gsend.at[k],
            dst_ref=grecv.at[k],
            send_sem=g_ss.at[k],
            recv_sem=g_rs.at[k],
            device_id=plane(lax.rem(me + k, group)),
            device_id_type=MESH,
        )

    def make_piece(k):
        to = lax.rem(me + k, group)
        lhs = scaled[to // n_col]
        cols = pl.ds(pl.multiple_of((to % n_col) * piece, hd), piece)
        for h in range(2):
            gsend[k, h] = jnp.dot(lhs, wgu[h, :, cols], preferred_element_type=F32).astype(BF16)

    @pl.loop(1, group)
    def _(k):
        make_piece(k)
        g_copy(k).start()

    make_piece(0)
    my_row = me // n_col
    sq_total = ssend[my_row]
    for k in range(1, group):
        s_copy(k).wait_recv()
        sq_total = sq_total + srecv[k - 1, my_row]
    norm = lax.rsqrt(sq_total / full_width + 1e-05)[:, 0:1]
    for k in range(1, group):
        g_copy(k).wait_recv()
    gate = gsend[0, 0].astype(F32)
    up = gsend[0, 1].astype(F32)
    for k in range(1, group):
        gate = gate + grecv[k, 0].astype(F32)
        up = up + grecv[k, 1].astype(F32)
    gate = gate * norm
    up = up * norm
    activated = (gate / (1.0 + jnp.exp(-gate)) * up).astype(BF16)
    asend[...] = activated

    def a_copy(k):
        return pltpu.make_async_remote_copy(
            src_ref=asend,
            dst_ref=act_all.at[k],
            send_sem=a_ss.at[k],
            recv_sem=a_rs.at[k],
            device_id=plane(lax.rem(me + k, group)),
            device_id_type=MESH,
        )

    for k in range(1, group):
        a_copy(k).start()
    loads[5].wait()
    down_acc[...] = jnp.zeros_like(down_acc)

    def add_piece(k, lhs):
        source = lax.rem(me - k + group, group)
        depth = pl.ds(pl.multiple_of((source % n_col) * piece, hd), piece)
        r = source // n_col
        down_acc[r] += jnp.dot(lhs, wd[depth, :], preferred_element_type=F32)

    add_piece(0, asend[...])

    @pl.loop(1, group)
    def _(k):
        a_copy(k).wait_recv()
        add_piece(k, act_all[k])

    lowered = down_acc[...].reshape(rows, width)
    out[...] = (hidden[...].astype(F32) + tensor_sum(1, lowered)).astype(BF16)

    for k in range(1, group):
        q_copy(k).wait_send()
        h_copy(k).wait_send()
        s_copy(k).wait_send()
        g_copy(k).wait_send()
        a_copy(k).wait_send()
    for k in range(1, n_tensor):
        z_copy(0, k).wait_send()
        z_copy(1, k).wait_send()


def body(
    dims,
    tokens,
    attn_gain,
    qkv_weight,
    qkv_order,
    cache_keys,
    cache_values,
    cache_len,
    out_weight,
    ffn_gain,
    gate_up,
    down_weight,
):
    n_section, n_dp, n_tensor = dims
    group = n_section * n_dp
    rows, width = tokens.shape
    seqs, groups, length, hd = cache_keys.shape
    qcols = qkv_weight.shape[1]
    units = gate_up.shape[2]
    n_col = math.gcd(group, units // hd)
    n_row = group // n_col
    row_part = rows // n_row
    piece = units // n_col
    n_heads_cols = out_weight.shape[0]

    half = hd // 2
    inv_freq = 500000.0 ** (-(2.0 * jnp.arange(half, dtype=F32)) / hd)
    angles = cache_len.astype(F32)[:, None] * inv_freq[None, :]
    cosine = jnp.cos(angles)
    sine = jnp.sin(angles)
    cos_full = jnp.concatenate([cosine, cosine], axis=1)
    sin_full = jnp.concatenate([-sine, sine], axis=1)

    vmem = pl.BlockSpec(memory_space=pltpu.VMEM)
    smem = pl.BlockSpec(memory_space=pltpu.SMEM)
    hbm = pl.BlockSpec(memory_space=pltpu.HBM)
    dma = pltpu.SemaphoreType.DMA
    peers = group - 1
    return pl.pallas_call(
        functools.partial(layer_kernel, dims),
        out_shape=jax.ShapeDtypeStruct((rows, width), BF16),
        in_specs=[smem, smem] + [vmem] * 5 + [hbm] * 6,
        out_specs=vmem,
        scratch_shapes=[
            pltpu.VMEM(qkv_weight.shape, BF16),
            pltpu.VMEM(cache_keys.shape, BF16),
            pltpu.VMEM(cache_values.shape, BF16),
            pltpu.VMEM(out_weight.shape, BF16),
            pltpu.VMEM(gate_up.shape, BF16),
            pltpu.VMEM(down_weight.shape, BF16),
            dma((6,)),
            pltpu.VMEM((group, seqs, qcols + hd), F32),
            pltpu.VMEM((peers, seqs, qcols + hd), F32),
            pltpu.VMEM((seqs, groups, 16, hd), F32),
            pltpu.VMEM((seqs, n_heads_cols), F32),
            pltpu.VMEM((group, seqs, n_heads_cols), F32),
            pltpu.VMEM((rows, n_heads_cols), F32),
            pltpu.VMEM((2, rows, width), BF16),
            pltpu.VMEM((2, n_tensor, rows, width), BF16),
            pltpu.VMEM((rows, width), BF16),
            pltpu.VMEM((n_row, row_part, width), BF16),
            pltpu.VMEM((n_row, row_part, hd), F32),
            pltpu.VMEM((peers, n_row, row_part, hd), F32),
            pltpu.VMEM((group, 2, row_part, piece), BF16),
            pltpu.VMEM((group, 2, row_part, piece), BF16),
            pltpu.VMEM((row_part, piece), BF16),
            pltpu.VMEM((group, row_part, piece), BF16),
            pltpu.VMEM((n_row, row_part, width), F32),
            dma((peers,)),
            dma((peers,)),
            dma((peers,)),
            dma((peers,)),
            dma((2, n_tensor - 1)),
            dma((2, n_tensor - 1)),
            dma((peers,)),
            dma((peers,)),
            dma((group,)),
            dma((group,)),
            dma((group,)),
            dma((group,)),
        ],
        compiler_params=pltpu.CompilerParams(
            collective_id=0, has_side_effects=True, vmem_limit_bytes=62 * 1024 * 1024
        ),
    )(
        qkv_order,
        cache_len,
        tokens,
        attn_gain[None, :],
        ffn_gain[None, :],
        cos_full,
        sin_full,
        qkv_weight,
        cache_keys,
        cache_values,
        out_weight,
        gate_up,
        down_weight,
    )


def solution(mesh):
    dims = (mesh.shape["section"], mesh.shape["dp"], mesh.shape["tensor"])
    return jax.shard_map(
        functools.partial(body, dims),
        mesh=mesh,
        in_specs=(
            P(None, ("section", "dp")),
            P(("section", "dp")),
            P(("section", "dp"), "tensor"),
            P(),
            P(("section", "dp"), "tensor", None, None),
            P(("section", "dp"), "tensor", None, None),
            P(("section", "dp")),
            P("tensor", ("section", "dp")),
            P(("section", "dp")),
            P(None, ("section", "dp"), "tensor"),
            P("tensor", ("section", "dp")),
        ),
        out_specs=P(None, ("section", "dp")),
        check_vma=False,
    )
```

```python
import functools
import math

import jax
import jax.numpy as jnp
import numpy as np
from jax import lax
from jax.experimental import pallas as pl
from jax.experimental.pallas import tpu as pltpu
from jax.sharding import PartitionSpec as P

MESH = pl.DeviceIdType.MESH
F32 = jnp.float32
BF16 = jnp.bfloat16
NT = (((1,), (1,)), ((), ()))


def layer_kernel(
    dims,
    order,
    lens,
    tokens,
    gain1,
    gain2,
    freq,
    wq_hbm,
    ck_hbm,
    cv_hbm,
    wo_hbm,
    wgu_hbm,
    wd_hbm,
    out,
    wq,
    ck,
    cv,
    wo,
    wgu,
    wd,
    load_sem,
    qsend,
    qrecv,
    nsend,
    nrecv,
    lbuf,
    att,
    att_send,
    heads_all,
    heads_full,
    zsend,
    zrecv,
    hidden,
    scaled,
    ssend,
    srecv,
    gsend,
    grecv,
    asend,
    act_all,
    down_acc,
    q_ss,
    q_rs,
    n_ss,
    n_rs,
    h_ss,
    h_rs,
    z_ss,
    z_rs,
    s_ss,
    s_rs,
    g_ss,
    g_rs,
    a_ss,
    a_rs,
):
    n_section, n_dp, n_tensor = dims
    group = n_section * n_dp
    me = lax.axis_index("section") * n_dp + lax.axis_index("dp")
    t_me = lax.axis_index("tensor")
    rows, width = tokens.shape
    full_width = width * group
    seqs, groups, length, hd = ck.shape
    qcols = wq.shape[1]
    blocks = qcols // (groups * hd)
    per_group = blocks - 2
    n_row, row_part = scaled.shape[0], scaled.shape[1]
    n_col = group // n_row
    piece = asend.shape[1]

    def plane(index):
        return {"section": index // n_dp, "dp": index % n_dp}

    loads = [
        pltpu.make_async_copy(src, dst, load_sem.at[i])
        for i, (src, dst) in enumerate(
            (
                (wq_hbm, wq),
                (ck_hbm, ck),
                (cv_hbm, cv),
                (wo_hbm, wo),
                (wgu_hbm, wgu),
                (wd_hbm, wd),
            )
        )
    ]
    loads[0].start()
    loads[1].start()

    barrier = pltpu.get_barrier_semaphore()
    for k in range(1, group):
        pl.semaphore_signal(
            barrier, inc=1, device_id=plane(lax.rem(me + k, group)), device_id_type=MESH
        )
    for k in range(1, n_tensor):
        pl.semaphore_signal(
            barrier, inc=1, device_id={"tensor": lax.rem(t_me + k, n_tensor)}, device_id_type=MESH
        )

    x = tokens[...].astype(F32)
    squares = jnp.sum(x * x, axis=1, keepdims=True)
    xg = (x * gain1[...]).astype(BF16)
    sq_lanes = jnp.broadcast_to(squares, (rows, hd))
    for p in range(group):
        nsend[p] = sq_lanes[p * seqs : (p + 1) * seqs]
    angle = [lens[b].astype(F32) * freq[...] for b in range(seqs)]
    lane = lax.broadcasted_iota(jnp.int32, (1, hd), 1)
    cosine = [jnp.cos(a) for a in angle]
    sine = [jnp.where(lane < hd // 2, -jnp.sin(a), jnp.sin(a)) for a in angle]
    loads[0].wait()
    for load in loads[2:]:
        load.start()
    part = jnp.dot(xg, wq[...], preferred_element_type=F32)
    for p in range(group):
        qsend[p] = part[p * seqs : (p + 1) * seqs].astype(BF16)

    def q_copy(k):
        to = lax.rem(me + k, group)
        return pltpu.make_async_remote_copy(
            src_ref=qsend.at[to],
            dst_ref=qrecv.at[k - 1],
            send_sem=q_ss.at[k - 1],
            recv_sem=q_rs.at[k - 1],
            device_id=plane(to),
            device_id_type=MESH,
        )

    def n_copy(k):
        to = lax.rem(me + k, group)
        return pltpu.make_async_remote_copy(
            src_ref=nsend.at[to],
            dst_ref=nrecv.at[k - 1],
            send_sem=n_ss.at[k - 1],
            recv_sem=n_rs.at[k - 1],
            device_id=plane(to),
            device_id_type=MESH,
        )

    pl.semaphore_wait(barrier, group - 1 + n_tensor - 1)
    for k in range(1, group):
        n_copy(k).start()
        q_copy(k).start()
    squares = nsend[me]
    for k in range(1, group):
        n_copy(k).wait_recv()
        squares = squares + nrecv[k - 1]
    factor = lax.rsqrt(squares / full_width + 1e-05)
    total = qsend[me].astype(F32)
    for k in range(1, group):
        q_copy(k).wait_recv()
        total = total + qrecv[k - 1].astype(F32)
    for g in range(groups):
        stored = [
            total[:, (g * blocks + j) * hd : (g * blocks + j + 1) * hd] * factor
            for j in range(blocks)
        ]
        for i in range(blocks):
            logical = jnp.zeros((seqs, hd), F32)
            for j in range(blocks):
                logical = logical + jnp.where(order[j] == i, 1.0, 0.0).astype(F32) * stored[j]
            for b in range(seqs):
                lbuf[b, g, i : i + 1, :] = logical[b : b + 1]

    loads[1].wait()
    loads[2].wait()
    inv_scale = 1.0 / math.sqrt(hd)
    column = lax.broadcasted_iota(jnp.int32, (per_group, length), 1)

    def turn(vec, b):
        return vec * cosine[b] + pltpu.roll(vec, hd // 2, 1) * sine[b]

    for b in range(seqs):
        for g in range(groups):
            q = turn(lbuf[b, g, :per_group, :], b).astype(BF16)
            both = lbuf[b, g, per_group : per_group + 8, :]
            nk = turn(both, b).astype(BF16).astype(F32)[0:1]
            nv = both.astype(BF16).astype(F32)[1:2]
            scores = lax.dot_general(q, ck[b, g], NT, preferred_element_type=F32) * inv_scale
            own = jnp.sum(q.astype(F32) * nk, axis=1, keepdims=True) * inv_scale
            scores = jnp.where(column < lens[b], scores, -jnp.inf)
            peak = jnp.maximum(jnp.max(scores, axis=1, keepdims=True), own)
            weights = jnp.exp(scores - peak)
            own_w = jnp.exp(own - peak)
            denom = jnp.sum(weights, axis=1, keepdims=True) + own_w
            mixed = jnp.dot(weights.astype(BF16), cv[b, g], preferred_element_type=F32)
            mixed = (mixed + own_w * nv) / denom
            for i in range(per_group):
                at = (g * per_group + i) * hd
                att[b : b + 1, at : at + hd] = mixed[i : i + 1]

    def h_copy(k):
        return pltpu.make_async_remote_copy(
            src_ref=att_send,
            dst_ref=heads_all.at[me],
            send_sem=h_ss.at[k - 1],
            recv_sem=h_rs.at[k - 1],
            device_id=plane(lax.rem(me + k, group)),
            device_id_type=MESH,
        )

    att_send[...] = att[...].astype(BF16)
    for k in range(1, group):
        h_copy(k).start()
    heads_all[me] = att_send[...]
    loads[3].wait()
    for k in range(1, group):
        h_copy(k).wait_recv()
    for p in range(group):
        heads_full[p * seqs : (p + 1) * seqs, :] = heads_all[p].astype(F32)

    def z_copy(stage, k):
        return pltpu.make_async_remote_copy(
            src_ref=zsend.at[stage],
            dst_ref=zrecv.at[stage, t_me],
            send_sem=z_ss.at[stage, k - 1],
            recv_sem=z_rs.at[stage, k - 1],
            device_id={"tensor": lax.rem(t_me + k, n_tensor)},
            device_id_type=MESH,
        )

    def tensor_sum(stage, partial):
        rounded = partial.astype(BF16)
        zsend[stage] = rounded
        for k in range(1, n_tensor):
            z_copy(stage, k).start()
        zrecv[stage, t_me] = rounded
        for k in range(1, n_tensor):
            z_copy(stage, k).wait_recv()
        summed = zrecv[stage, 0].astype(F32)
        for t in range(1, n_tensor):
            summed = summed + zrecv[stage, t].astype(F32)
        return summed

    partial = jnp.dot(heads_full[...].astype(BF16), wo[...], preferred_element_type=F32)
    state = (tokens[...].astype(F32) + tensor_sum(0, partial)).astype(BF16)
    hidden[...] = state
    h32 = state.astype(F32)
    hsq = jnp.broadcast_to(jnp.sum(h32 * h32, axis=1, keepdims=True), (rows, hd))
    hgain = (h32 * gain2[...]).astype(BF16)
    for r in range(n_row):
        ssend[r] = hsq[r * row_part : (r + 1) * row_part]
        scaled[r] = hgain[r * row_part : (r + 1) * row_part]

    def s_copy(k):
        return pltpu.make_async_remote_copy(
            src_ref=ssend,
            dst_ref=srecv.at[k - 1],
            send_sem=s_ss.at[k - 1],
            recv_sem=s_rs.at[k - 1],
            device_id=plane(lax.rem(me + k, group)),
            device_id_type=MESH,
        )

    for k in range(1, group):
        s_copy(k).start()

    loads[4].wait()

    def g_copy(k):
        return pltpu.make_async_remote_copy(
            src_ref=gsend.at[k],
            dst_ref=grecv.at[k],
            send_sem=g_ss.at[k],
            recv_sem=g_rs.at[k],
            device_id=plane(lax.rem(me + k, group)),
            device_id_type=MESH,
        )

    def make_piece(k):
        to = lax.rem(me + k, group)
        lhs = scaled[to // n_col]
        cols = pl.ds(pl.multiple_of((to % n_col) * piece, hd), piece)
        for h in range(2):
            gsend[k, h] = jnp.dot(lhs, wgu[h, :, cols], preferred_element_type=F32).astype(BF16)

    @pl.loop(1, group)
    def _(k):
        make_piece(k)
        g_copy(k).start()

    make_piece(0)
    my_row = me // n_col
    sq_total = ssend[my_row]
    for k in range(1, group):
        s_copy(k).wait_recv()
        sq_total = sq_total + srecv[k - 1, my_row]
    norm = lax.rsqrt(sq_total / full_width + 1e-05)[:, 0:1]
    for k in range(1, group):
        g_copy(k).wait_recv()
    gate = gsend[0, 0].astype(F32)
    up = gsend[0, 1].astype(F32)
    for k in range(1, group):
        gate = gate + grecv[k, 0].astype(F32)
        up = up + grecv[k, 1].astype(F32)
    gate = gate * norm
    up = up * norm
    activated = (gate / (1.0 + jnp.exp(-gate)) * up).astype(BF16)
    asend[...] = activated

    def a_copy(k):
        return pltpu.make_async_remote_copy(
            src_ref=asend,
            dst_ref=act_all.at[k],
            send_sem=a_ss.at[k],
            recv_sem=a_rs.at[k],
            device_id=plane(lax.rem(me + k, group)),
            device_id_type=MESH,
        )

    for k in range(1, group):
        a_copy(k).start()
    loads[5].wait()
    down_acc[...] = jnp.zeros_like(down_acc)

    def add_piece(k, lhs):
        source = lax.rem(me - k + group, group)
        depth = pl.ds(pl.multiple_of((source % n_col) * piece, hd), piece)
        r = source // n_col
        down_acc[r] += jnp.dot(lhs, wd[depth, :], preferred_element_type=F32)

    add_piece(0, asend[...])

    @pl.loop(1, group)
    def _(k):
        a_copy(k).wait_recv()
        add_piece(k, act_all[k])

    lowered = down_acc[...].reshape(rows, width)
    out[...] = hidden[...].astype(F32) + tensor_sum(1, lowered)

    for k in range(1, group):
        n_copy(k).wait_send()
        q_copy(k).wait_send()
        h_copy(k).wait_send()
        s_copy(k).wait_send()
        g_copy(k).wait_send()
        a_copy(k).wait_send()
    for k in range(1, n_tensor):
        z_copy(0, k).wait_send()
        z_copy(1, k).wait_send()


def body(
    dims,
    tokens,
    attn_gain,
    qkv_weight,
    qkv_order,
    cache_keys,
    cache_values,
    cache_len,
    out_weight,
    ffn_gain,
    gate_up,
    down_weight,
):
    n_section, n_dp, n_tensor = dims
    group = n_section * n_dp
    rows, width = tokens.shape
    seqs, groups, length, hd = cache_keys.shape
    qcols = qkv_weight.shape[1]
    units = gate_up.shape[2]
    n_col = math.gcd(group, units // hd)
    n_row = group // n_col
    row_part = rows // n_row
    piece = units // n_col
    n_heads_cols = out_weight.shape[0]

    half = hd // 2
    inv_freq = 500000.0 ** (-(2.0 * np.arange(half)) / hd)
    freq = jnp.asarray(np.concatenate([inv_freq, inv_freq])[None, :], F32)

    vmem = pl.BlockSpec(memory_space=pltpu.VMEM)
    smem = pl.BlockSpec(memory_space=pltpu.SMEM)
    hbm = pl.BlockSpec(memory_space=pltpu.HBM)
    dma = pltpu.SemaphoreType.DMA
    peers = group - 1
    summed = pl.pallas_call(
        functools.partial(layer_kernel, dims),
        out_shape=jax.ShapeDtypeStruct((rows, width), F32),
        in_specs=[smem, smem] + [vmem] * 4 + [hbm] * 6,
        out_specs=vmem,
        scratch_shapes=[
            pltpu.VMEM(qkv_weight.shape, BF16),
            pltpu.VMEM(cache_keys.shape, BF16),
            pltpu.VMEM(cache_values.shape, BF16),
            pltpu.VMEM(out_weight.shape, BF16),
            pltpu.VMEM(gate_up.shape, BF16),
            pltpu.VMEM(down_weight.shape, BF16),
            dma((6,)),
            pltpu.VMEM((group, seqs, qcols), BF16),
            pltpu.VMEM((peers, seqs, qcols), BF16),
            pltpu.VMEM((group, seqs, hd), F32),
            pltpu.VMEM((peers, seqs, hd), F32),
            pltpu.VMEM((seqs, groups, 16, hd), F32),
            pltpu.VMEM((seqs, n_heads_cols), F32),
            pltpu.VMEM((seqs, n_heads_cols), BF16),
            pltpu.VMEM((group, seqs, n_heads_cols), BF16),
            pltpu.VMEM((rows, n_heads_cols), F32),
            pltpu.VMEM((2, rows, width), BF16),
            pltpu.VMEM((2, n_tensor, rows, width), BF16),
            pltpu.VMEM((rows, width), BF16),
            pltpu.VMEM((n_row, row_part, width), BF16),
            pltpu.VMEM((n_row, row_part, hd), F32),
            pltpu.VMEM((peers, n_row, row_part, hd), F32),
            pltpu.VMEM((group, 2, row_part, piece), BF16),
            pltpu.VMEM((group, 2, row_part, piece), BF16),
            pltpu.VMEM((row_part, piece), BF16),
            pltpu.VMEM((group, row_part, piece), BF16),
            pltpu.VMEM((n_row, row_part, width), F32),
            dma((peers,)),
            dma((peers,)),
            dma((peers,)),
            dma((peers,)),
            dma((peers,)),
            dma((peers,)),
            dma((2, n_tensor - 1)),
            dma((2, n_tensor - 1)),
            dma((peers,)),
            dma((peers,)),
            dma((group,)),
            dma((group,)),
            dma((group,)),
            dma((group,)),
        ],
        compiler_params=pltpu.CompilerParams(
            collective_id=0, has_side_effects=True, vmem_limit_bytes=62 * 1024 * 1024
        ),
    )(
        qkv_order,
        cache_len,
        tokens,
        attn_gain[None, :],
        ffn_gain[None, :],
        freq,
        qkv_weight,
        cache_keys,
        cache_values,
        out_weight,
        gate_up,
        down_weight,
    )
    return summed.astype(BF16)


def solution(mesh):
    dims = (mesh.shape["section"], mesh.shape["dp"], mesh.shape["tensor"])
    return jax.shard_map(
        functools.partial(body, dims),
        mesh=mesh,
        in_specs=(
            P(None, ("section", "dp")),
            P(("section", "dp")),
            P(("section", "dp"), "tensor"),
            P(),
            P(("section", "dp"), "tensor", None, None),
            P(("section", "dp"), "tensor", None, None),
            P(("section", "dp")),
            P("tensor", ("section", "dp")),
            P(("section", "dp")),
            P(None, ("section", "dp"), "tensor"),
            P("tensor", ("section", "dp")),
        ),
        out_specs=P(None, ("section", "dp")),
        check_vma=False,
    )
```
